32 devices in a mesh: grp: 2 (over x), dev: 16 (over z, y, core).
Axes of the slice: x: 2, y: 2, z: 4, core: 2. Of those that a mesh axis runs over, the one named last changes fastest.
Arguments:
- frames: float32 [2, 128, 512, 512], P('grp', 'dev'), may hold values from -6 to 6
- ref_spectrum: float32 [2, 128, 512, 512], P(None, None, 'dev'), as said below
- shifts: int32 [2, 3], replicated, may hold values from 0 to 127
- offsets: int32 [2, 3], replicated, may hold values from 0 to 127
Outputs:
- correlation: float32 [2, 128, 128, 128], P('grp', 'dev')
- new_reference: float32 [2, 128, 512, 512], P(None, 'grp', 'dev')
The draws below stay inside these ranges and needn't reach their ends.
Inputs may be any that keep to these rules, and one draw needn't show every extreme that they name: `ref_spectrum`: real and imaginary parts are real numbers.
All inputs are finite; a program needn't handle non-finite values.
Results may differ from the reference program's by a relative error of at most 0.0001.
Values sent between devices are 32-bit elements; how exact they have to be, the bound alone decides.
No kernel may reach another device: no remote copies, remote signals or barrier semaphores. Data moves between devices by JAX's collectives and lax.ppermute only.
A program may use at most 192 MiB of HBM per device.

```python
import math
import jax
import jax.numpy as jnp

NX = 512
NY = 512
NZ = 128
CROP = 128
TIMES = 2


def draw_ref_spectrum(key, part):
    first, second = jax.random.split(key)
    base = jax.random.normal(first, (2, NZ, NY, NX), jnp.float32)
    spread = 10.0
    rows = jnp.arange(NY, dtype=jnp.float32) / (NY - 1)
    row_scale = spread ** (rows - 0.5)
    column_scale = jnp.exp(jax.random.uniform(second, (NX,), jnp.float32, 0.0, math.log(3.0)))
    return base * row_scale[None, None, :, None] * column_scale[None, None, None, :]


def with_ends(result, stream_key, low, top_value):
    longest = result.shape.index(max(result.shape))
    spots = []
    for shift in (0, 1):
        where = [jax.random.randint(jax.random.fold_in(stream_key, axis), (), 0, length) for axis, length in enumerate(result.shape)]
        where[longest] = (where[longest] + shift) % result.shape[longest]
        spots.append(tuple(where))
    return result.at[spots[0]].set(low).at[spots[1]].set(top_value)


def levels(own_key, dims, shards, low, top_value):
    loudness, own = 1.0, jax.random.fold_in(own_key, 6)
    for position, shards_of in shards:
        steps = jnp.exp(jax.random.uniform(jax.random.fold_in(own, position), (shards_of,), jnp.float32, low / len(shards), top_value / len(shards)))
        loudness = loudness * jnp.repeat(steps, dims[position] // shards_of).reshape([-1 if axis == position else 1 for axis in range(len(dims))])
    return loudness


def normal_values(key, dims, scale, reach, shards=(), kind=jnp.bfloat16):
    loudness = levels(key, dims, shards, -0.22, 0.18) if shards else 1.0
    array = jax.random.normal(key, dims, jnp.float32) * scale * loudness
    return jnp.minimum(jnp.maximum(array, -reach), reach).astype(kind)


def setup_inputs(seed: int = 0) -> dict:
    arg_keys = jax.random.split(jax.random.key(seed), 5)
    return {
        "frames": normal_values(arg_keys[0], (TIMES, NZ, NY, NX), 1.0, 6.0, ((0, 2), (1, 16)), jnp.float32),
        "ref_spectrum": draw_ref_spectrum(jax.random.fold_in(arg_keys[4], 71), 0),
        "shifts": with_ends(jax.random.randint(arg_keys[2], (TIMES, 3), 0, NZ), jax.random.fold_in(arg_keys[2], 1), 0, NZ - 1).astype(jnp.int32),
        "offsets": with_ends(jax.random.randint(arg_keys[3], (TIMES, 3), 0, NZ), jax.random.fold_in(arg_keys[3], 1), 0, NZ - 1).astype(jnp.int32),
    }


def reference(frames, ref_spectrum, shifts, offsets):
    total = NZ * NY * NX
    root = math.sqrt(total)
    spectrum_ref = ref_spectrum[0] + 1j * ref_spectrum[1]
    results = []
    warped_sum = jnp.zeros_like(spectrum_ref)
    for timepoint in range(TIMES):
        frame = frames[timepoint]
        spectrum = jnp.fft.fftn(frame) / root
        cross = spectrum * jnp.conj(spectrum_ref)
        magnitude = jnp.abs(cross)
        average = jnp.sum(magnitude) / total
        whitened = cross / (magnitude + average)
        field = jnp.real(jnp.fft.ifftn(whitened)) * root
        offset = offsets[timepoint]
        index_z = ((offset[0] + jnp.arange(CROP, dtype=jnp.int32)) % NZ).astype(jnp.int32)
        index_y = ((offset[1] + jnp.arange(CROP, dtype=jnp.int32)) % NY).astype(jnp.int32)
        index_x = ((offset[2] + jnp.arange(CROP, dtype=jnp.int32)) % NX).astype(jnp.int32)
        cropped = jnp.take(field, index_z, axis=0)
        cropped = jnp.take(cropped, index_y, axis=1)
        cropped = jnp.take(cropped, index_x, axis=2)
        results.append(cropped.astype(jnp.float32))
        drift = shifts[timepoint]
        moved = jnp.roll(frame, (drift[0], drift[1], drift[2]), axis=(0, 1, 2))
        warped_sum = warped_sum + jnp.fft.fftn(moved) / root
    updated = 0.5 * spectrum_ref + 0.25 * warped_sum
    new_reference = jnp.stack([jnp.real(updated), jnp.imag(updated)]).astype(jnp.float32)
    return (jnp.stack(results), new_reference)
```

```python
import functools
import math

import jax
import jax.numpy as jnp
import ml_dtypes
import numpy as np
from jax import lax
from jax.experimental import pallas as pl
from jax.experimental.pallas import tpu as pltpu
from jax.sharding import PartitionSpec as P

CROP = 128
LANES = 128
ROWS = 8
F32 = jnp.float32
BF16 = jnp.bfloat16


def fixed_wave(length):
    phases = np.outer(np.arange(length), np.arange(length)) % length
    angles = 2.0 * np.pi / length * phases
    table = np.concatenate([np.cos(angles), np.sin(angles)], 0).astype(np.float32)
    high = table.astype(ml_dtypes.bfloat16)
    low = (table - high.astype(np.float32)).astype(ml_dtypes.bfloat16)
    return np.stack([high, low])


def wave(rows, columns, length):
    phases = rows[:, None] * columns[None, :] % length
    angles = 2.0 * math.pi / length * phases.astype(F32)
    return (jnp.cos(angles), jnp.sin(angles))


def ramp(index, drift, length):
    angles = 2.0 * math.pi / length * (index * drift % length).astype(F32)
    return (jnp.cos(angles), jnp.sin(angles))


def halves(table):
    high = lax.reduce_precision(table, 8, 7)
    return jnp.stack([high.astype(BF16), (table - high).astype(BF16)])


def parts(value):
    high = value.astype(BF16)
    return high, (value - high.astype(F32)).astype(BF16)


def dot3(left, right):
    return jnp.dot(
        jnp.concatenate([left[0], left[0], left[1]], 1),
        jnp.concatenate([right[0], right[1], right[0]], 0),
        preferred_element_type=F32,
    )


def forward_kernel(frame, table_x, table_y, *refs):
    out = refs[-1]
    count, ny, nx = frame.shape
    devices, _, _, rows, _ = out.shape
    column = [jnp.concatenate([table_x[i, :nx, :], table_x[i, nx:, :]], 1) for i in range(2)]
    for z in range(count):
        plane = parts(dot3(parts(frame[z]), column))
        both = dot3((table_y[0], table_y[1]), plane)
        real = both[:ny, :LANES] - both[ny:, LANES:]
        imag = -both[:ny, LANES:] - both[ny:, :LANES]
        out[:, 0, z] = real.reshape(devices, rows, LANES)
        out[:, 1, z] = imag.reshape(devices, rows, LANES)


def middle_kernel(group, got, table, ref_own, ref_far, turn_z, turn_yx, cross, size, own, far, sums):
    del group
    nz = cross.shape[2]
    half = own.shape[1]
    flat = got.reshape(2 * nz * ROWS, LANES)
    near = ref_own.reshape(2 * half * ROWS, LANES)
    away = ref_far.reshape(2 * half * ROWS, LANES)
    own_flat = own.reshape(2 * half * ROWS, LANES)
    far_flat = far.reshape(2 * half * ROWS, LANES)
    matrix = (table[0], table[1])
    zc, zs = turn_z[0], turn_z[1]
    total = jnp.zeros((8, LANES), F32)
    for pair in range(0, ROWS, 2):
        taken = [flat[pl.ds(r, 2 * nz, stride=ROWS), :] for r in (pair, pair + 1)]
        freq = dot3(matrix, parts(jnp.concatenate(taken, 1)))
        for r in (pair, pair + 1):
            at = slice((r - pair) * LANES, (r - pair + 1) * LANES)
            fr, fi = freq[:nz, at], freq[nz:, at]
            yc, ys = turn_yx[0, r : r + 1, :], turn_yx[1, r : r + 1, :]
            ar, ai = fr * zc + fi * zs, fi * zc - fr * zs
            wr, wi = ar * yc + ai * ys, ai * yc - ar * ys
            own_part = [near[pl.ds(p * half * ROWS + r, half, stride=ROWS), :] for p in range(2)]
            far_part = [away[pl.ds(p * half * ROWS + r, half, stride=ROWS), :] for p in range(2)]
            for p, w in enumerate((wr, wi)):
                where = pl.ds(p * half * ROWS + r, half, stride=ROWS)
                own_flat[where, :] = w[:half] + 0.5 * own_part[p]
                far_flat[where, :] = w[half:]
            rr = jnp.concatenate([own_part[0], far_part[0]], 0)
            ri = jnp.concatenate([own_part[1], far_part[1]], 0)
            cr = fr * rr + fi * ri
            ci = fi * rr - fr * ri
            cross[r, 0] = cr
            cross[r, 1] = ci
            magnitude = jnp.sqrt(cr * cr + ci * ci)
            size[r] = magnitude
            total = total + jnp.sum(magnitude.reshape(nz // 8, 8, LANES), 0)
    sums[0] = total


def inverse_kernel(average, *refs):
    table_x, table_z, out = refs[-3:]
    crosses, sizes = refs[: len(refs) // 2 - 1], refs[len(refs) // 2 - 1 : -3]
    nz = crosses[0].shape[2]
    mean = average[0]
    flat = out.reshape(2 * CROP * ROWS, LANES)
    matrix = (table_z[0], table_z[1])
    width = None
    for c, (cross, size) in enumerate(zip(crosses, sizes)):
        scale = 1.0 / (size[...] + mean)
        white = jnp.concatenate(
            [(cross[:, p] * scale).reshape(ROWS * nz, LANES) for p in range(2)], 1
        )
        at = slice(c * 2 * LANES, (c + 1) * 2 * LANES)
        piece = dot3(parts(white), (table_x[0, at, :], table_x[1, at, :]))
        width = piece if width is None else width + piece
    for pair in range(0, ROWS, 2):
        stacked = jnp.concatenate(
            [
                jnp.concatenate([width[r * nz : (r + 1) * nz, :CROP], width[r * nz : (r + 1) * nz, CROP:]], 0)
                for r in (pair, pair + 1)
            ],
            1,
        )
        depth = dot3(matrix, parts(stacked))
        flat[pl.ds(pair, 2 * CROP, stride=ROWS), :] = depth[:, :CROP]
        flat[pl.ds(pair + 1, 2 * CROP, stride=ROWS), :] = depth[:, CROP:]


def total_over(value, axis, size):
    if size & (size - 1):
        return lax.psum(value, axis)
    step = 1
    while step < size:
        flips = (1, 2, 3) if 2 * step < size else (1,)
        pairs = [[(i, i ^ (flip * step)) for i in range(size)] for flip in flips]
        value = value + sum(lax.ppermute(value, axis, pair) for pair in pairs)
        step *= len(flips) + 1
    return value


def local(frames, ref_spectrum, shifts, offsets, *, groups, devices):
    group = lax.axis_index("grp")
    device = lax.axis_index("dev")
    _, planes, ny, nx = frames.shape
    _, nz, rows, _ = ref_spectrum.shape
    total = nz * ny * nx
    factor = 1.0 / math.sqrt(total)
    half = nz // groups
    chunks = nx // LANES
    frame = frames[0]
    ints = lambda count: jnp.arange(count, dtype=jnp.int32)
    whole = lambda shape: pl.BlockSpec(shape, lambda *_: (0,) * len(shape))

    table_x = jnp.asarray(fixed_wave(nx))
    table_y = table_x if ny == nx else jnp.asarray(fixed_wave(ny))

    def send(c, *after):
        return pl.pallas_call(
            forward_kernel,
            grid=(planes // 2,),
            in_specs=[
                pl.BlockSpec((2, ny, nx), lambda z: (z, 0, 0)),
                pl.BlockSpec((2, 2 * nx, LANES), lambda z: (0, 0, c)),
                whole((2, 2 * ny, ny)),
            ]
            + [pl.BlockSpec(memory_space=pl.ANY)] * len(after),
            out_specs=pl.BlockSpec((devices, 2, 2, rows, LANES), lambda z: (0, 0, z, 0, 0)),
            out_shape=jax.ShapeDtypeStruct((devices, 2, planes, rows, LANES), F32),
            name=f"forward_{c}",
        )(frame, table_x, table_y, *after)

    def exchange(packed):
        return lax.all_to_all(packed, "dev", split_axis=0, concat_axis=0, tiled=True)

    first = send(0)
    shifts, offsets, first = lax.optimization_barrier((shifts, offsets, first))
    drift = lax.dynamic_index_in_dim(shifts, group, 0, keepdims=False)
    corner = lax.dynamic_index_in_dim(offsets, group, 0, keepdims=False)
    kz = (ints(nz) + group * half) % nz
    ky = device * rows + ints(rows)
    cos_z, sin_z = wave(kz, ints(nz), nz)
    split = lambda table: table.reshape(nz, devices, planes)
    table_z = halves(
        factor
        * jnp.stack(
            [
                jnp.stack([split(cos_z), split(sin_z)], 2),
                jnp.stack([-split(sin_z), split(cos_z)], 2),
            ]
        ).reshape(2 * nz, 2 * nz)
    )
    cz, sz = ramp(kz, drift[0], nz)
    turn_z = jnp.broadcast_to(jnp.stack([cz, sz])[:, :, None], (2, nz, LANES))
    cy, sy = ramp(ky, drift[1], ny)
    cx, sx = ramp(ints(nx), drift[2], nx)
    turn_yx = 0.25 * jnp.stack(
        [cy[:, None] * cx - sy[:, None] * sx, sy[:, None] * cx + cy[:, None] * sx]
    )
    ref_view = ref_spectrum.reshape(2, groups, half, rows, nx)
    group_number = group.astype(jnp.int32).reshape(1)
    steps = rows // ROWS

    def middle(got, c):
        return pl.pallas_call(
            middle_kernel,
            grid_spec=pltpu.PrefetchScalarGridSpec(
                num_scalar_prefetch=1,
                grid=(steps,),
                in_specs=[
                    pl.BlockSpec((2 * nz, ROWS, LANES), lambda i, g: (0, i, 0)),
                    whole((2, 2 * nz, 2 * nz)),
                    pl.BlockSpec((2, 1, half, ROWS, LANES), lambda i, g: (0, g[0], 0, i, c)),
                    pl.BlockSpec((2, 1, half, ROWS, LANES), lambda i, g: (0, groups - 1 - g[0], 0, i, c)),
                    whole((2, nz, LANES)),
                    pl.BlockSpec((2, ROWS, LANES), lambda i, g: (0, i, c)),
                ],
                out_specs=[
                    pl.BlockSpec((ROWS, 2, nz, LANES), lambda i, g: (i, 0, 0, 0)),
                    pl.BlockSpec((ROWS, nz, LANES), lambda i, g: (i, 0, 0)),
                    pl.BlockSpec((2, half, ROWS, LANES), lambda i, g: (0, 0, i, 0)),
                    pl.BlockSpec((2, half, ROWS, LANES), lambda i, g: (0, 0, i, 0)),
                    pl.BlockSpec((1, 8, LANES), lambda i, g: (i, 0, 0)),
                ],
            ),
            out_shape=[
                jax.ShapeDtypeStruct((rows, 2, nz, LANES), F32),
                jax.ShapeDtypeStruct((rows, nz, LANES), F32),
                jax.ShapeDtypeStruct((2, half, rows, LANES), F32),
                jax.ShapeDtypeStruct((2, half, rows, LANES), F32),
                jax.ShapeDtypeStruct((steps, 8, LANES), F32),
            ],
            name=f"middle_{c}",
        )(group_number, got, table_z, ref_view, ref_view, turn_z, turn_yx)

    crosses, sizes, owns, fars, sums = [], [], [], [], []
    swap = [(i, groups - 1 - i) for i in range(groups)]
    packed = [first]
    for c in range(chunks):
        if c + 1 < chunks:
            packed.append(send(c + 1, packed[c], *sums[-1:]))
        if c > 1:
            packed[c], fars[c - 2] = lax.optimization_barrier((packed[c], fars[c - 2]))
        got = exchange(packed[c]).reshape(2 * nz, rows, LANES)
        if c > 0 and c == chunks - 1:
            got, fars[c - 1] = lax.optimization_barrier((got, fars[c - 1]))
        cross, size, own, far, part = middle(got, c)
        sizes.append(size)
        crosses.append(cross)
        owns.append(own)
        fars.append(lax.ppermute(far, "grp", swap))
        sums.append(part)
    mass = jnp.sum(sum(sums))
    average = total_over(mass, "dev", devices) / total

    take_x = (ints(CROP) + corner[2]) % nx
    take_y = (ints(CROP) + corner[1]) % ny
    take_z = (ints(CROP) + corner[0]) % nz
    cb, sb = wave(ints(nx), take_x, nx)
    lanes = lambda table: table.reshape(chunks, LANES, CROP)
    cb, sb = lanes(cb), lanes(sb)
    back_x = halves(
        jnp.stack(
            [jnp.concatenate([cb, sb], 2), jnp.concatenate([-sb, cb], 2)], 1
        ).reshape(2 * nx, 2 * CROP)
    )
    bz, dz = wave(take_z, kz, nz)
    back_z = halves(
        jnp.stack(
            [jnp.concatenate([bz, -dz], 1), jnp.concatenate([dz, bz], 1)], 1
        ).reshape(2 * CROP, 2 * nz)
    )
    cos_b, sin_b = wave(take_y, ints(ny), ny)
    back_y = factor * jnp.stack(
        [cos_b.reshape(CROP, devices, rows), -sin_b.reshape(CROP, devices, rows)], 2
    )
    back = pl.pallas_call(
        inverse_kernel,
        grid=(steps,),
        in_specs=[pl.BlockSpec(memory_space=pltpu.SMEM)]
        + [pl.BlockSpec((ROWS, 2, nz, LANES), lambda i: (i, 0, 0, 0))] * chunks
        + [pl.BlockSpec((ROWS, nz, LANES), lambda i: (i, 0, 0))] * chunks
        + [whole((2, 2 * nx, 2 * CROP)), whole((2, 2 * CROP, 2 * nz))],
        out_specs=pl.BlockSpec((2 * CROP, ROWS, LANES), lambda i: (0, i, 0)),
        out_shape=jax.ShapeDtypeStruct((2 * CROP, rows, LANES), F32),
        name="inverse",
    )(average.reshape(1), *crosses, *sizes, back_x, back_z)
    slab = exchange(back.reshape(devices, CROP // devices, 2, rows, CROP))
    field = jnp.einsum("szprx,yspr->zyx", slab, back_y, precision=lax.Precision.HIGH)
    new_reference = jnp.concatenate([own + far for own, far in zip(owns, fars)], 3)
    return (field[None], new_reference)


def solution(mesh):
    body = functools.partial(local, groups=mesh.shape["grp"], devices=mesh.shape["dev"])
    return jax.shard_map(
        body,
        mesh=mesh,
        in_specs=(P("grp", "dev", None, None), P(None, None, "dev", None), P(), P()),
        out_specs=(P("grp", "dev", None, None), P(None, "grp", "dev", None)),
        check_vma=False,
    )
```

```python
import functools
import math

import jax
import jax.numpy as jnp
import ml_dtypes
import numpy as np
from jax import lax
from jax.experimental import pallas as pl
from jax.experimental.pallas import tpu as pltpu
from jax.sharding import PartitionSpec as P


CROP = 128
LANES = 128
ROWS = 8
F32 = jnp.float32
BF16 = jnp.bfloat16


def fixed_wave(length):
    phases = np.outer(np.arange(length), np.arange(length)) % length
    angles = 2.0 * np.pi / length * phases
    table = np.concatenate([np.cos(angles), np.sin(angles)], 0).astype(np.float32)
    high = table.astype(ml_dtypes.bfloat16)
    low = (table - high.astype(np.float32)).astype(ml_dtypes.bfloat16)
    return np.stack([high, low])


def wave(rows, columns, length):
    phases = rows[:, None] * columns[None, :] % length
    angles = 2.0 * math.pi / length * phases.astype(F32)
    return (jnp.cos(angles), jnp.sin(angles))


def ramp(index, drift, length):
    angles = 2.0 * math.pi / length * (index * drift % length).astype(F32)
    return (jnp.cos(angles), jnp.sin(angles))


def halves(table):
    high = lax.reduce_precision(table, 8, 7)
    return jnp.stack([high.astype(BF16), (table - high).astype(BF16)])


def parts(value):
    high = value.astype(BF16)
    return high, (value - high.astype(F32)).astype(BF16)


def dot3(left, right):
    return jnp.dot(
        jnp.concatenate([left[0], left[0], left[1]], 1),
        jnp.concatenate([right[0], right[1], right[0]], 0),
        preferred_element_type=F32,
    )


def forward_kernel(device, frame, table_x, table_y, *refs, partners):
    outs, scratch = refs[-1 - partners : -1], refs[-1]
    count, ny, nx = frame.shape
    rows = outs[0].shape[2]
    column = [jnp.concatenate([table_x[i, :nx, :], table_x[i, nx:, :]], 1) for i in range(2)]
    for z in range(count):
        plane = parts(dot3(parts(frame[z]), column))
        both = dot3((table_y[0], table_y[1]), plane)
        scratch[z, 0] = both[:ny, :LANES] - both[ny:, LANES:]
        scratch[z, 1] = -both[:ny, LANES:] - both[ny:, :LANES]
    for k, out in enumerate(outs):
        at = pl.ds(pl.multiple_of((device[0] ^ k) * rows, rows), rows)
        for z in range(count):
            out[0, z] = scratch[z, 0, at, :]
            out[1, z] = scratch[z, 1, at, :]


def middle_kernel(group, *refs, partners, after):
    del group
    refs = refs[:partners] + refs[partners + after :]
    gots, (table, ref_own, ref_far, turn_z, turn_yx, cross, size, own, far, sums) = refs[:-10], refs[-10:]
    each = gots[0].shape[0]
    nz = cross.shape[2]
    half = own.shape[1]
    flats = [got.reshape(each * ROWS, LANES) for got in gots]
    near = ref_own.reshape(2 * half * ROWS, LANES)
    away = ref_far.reshape(2 * half * ROWS, LANES)
    own_flat = own.reshape(2 * half * ROWS, LANES)
    far_flat = far.reshape(2 * half * ROWS, LANES)
    matrix = (table[0], table[1])
    zc, zs = turn_z[0], turn_z[1]
    total = jnp.zeros((8, LANES), F32)
    for pair in range(0, ROWS, 2):
        taken = [
            jnp.concatenate([flat[pl.ds(r, each, stride=ROWS), :] for flat in flats], 0)
            for r in (pair, pair + 1)
        ]
        freq = dot3(matrix, parts(jnp.concatenate(taken, 1)))
        for r in (pair, pair + 1):
            at = slice((r - pair) * LANES, (r - pair + 1) * LANES)
            fr, fi = freq[:nz, at], freq[nz:, at]
            yc, ys = turn_yx[0, r : r + 1, :], turn_yx[1, r : r + 1, :]
            ar, ai = fr * zc + fi * zs, fi * zc - fr * zs
            wr, wi = ar * yc + ai * ys, ai * yc - ar * ys
            own_part = [near[pl.ds(p * half * ROWS + r, half, stride=ROWS), :] for p in range(2)]
            far_part = [away[pl.ds(p * half * ROWS + r, half, stride=ROWS), :] for p in range(2)]
            for p, w in enumerate((wr, wi)):
                where = pl.ds(p * half * ROWS + r, half, stride=ROWS)
                own_flat[where, :] = w[:half] + 0.5 * own_part[p]
                far_flat[where, :] = w[half:]
            rr = jnp.concatenate([own_part[0], far_part[0]], 0)
            ri = jnp.concatenate([own_part[1], far_part[1]], 0)
            cr = fr * rr + fi * ri
            ci = fi * rr - fr * ri
            cross[r, 0] = cr
            cross[r, 1] = ci
            magnitude = jnp.sqrt(cr * cr + ci * ci)
            size[r] = magnitude
            total = total + jnp.sum(magnitude.reshape(nz // 8, 8, LANES), 0)
    sums[0] = total


def inverse_kernel(average, *refs, chunks):
    crosses, sizes = refs[:chunks], refs[chunks : 2 * chunks]
    table_x, table_z = refs[2 * chunks : 2 * chunks + 2]
    outs = refs[2 * chunks + 2 :]
    each = outs[0].shape[0]
    nz = crosses[0].shape[2]
    mean = average[0]
    flats = [out.reshape(each * ROWS, LANES) for out in outs]
    matrix = (table_z[0], table_z[1])
    width = None
    for c, (cross, size) in enumerate(zip(crosses, sizes)):
        scale = 1.0 / (size[...] + mean)
        white = jnp.concatenate(
            [(cross[:, p] * scale).reshape(ROWS * nz, LANES) for p in range(2)], 1
        )
        at = slice(c * 2 * LANES, (c + 1) * 2 * LANES)
        piece = dot3(parts(white), (table_x[0, at, :], table_x[1, at, :]))
        width = piece if width is None else width + piece
    for pair in range(0, ROWS, 2):
        stacked = jnp.concatenate(
            [
                jnp.concatenate([width[r * nz : (r + 1) * nz, :CROP], width[r * nz : (r + 1) * nz, CROP:]], 0)
                for r in (pair, pair + 1)
            ],
            1,
        )
        depth = dot3(matrix, parts(stacked))
        for k, flat in enumerate(flats):
            at = slice(k * each, (k + 1) * each)
            flat[pl.ds(pair, each, stride=ROWS), :] = depth[at, :CROP]
            flat[pl.ds(pair + 1, each, stride=ROWS), :] = depth[at, CROP:]


def partial_kernel(table, *refs, near):
    slabs, out = refs[:near], refs[-1]
    planes = out.shape[1]
    matrix = (table[0], table[1])
    for z in range(0, planes, 2):
        stacked = jnp.concatenate(
            [
                jnp.concatenate(
                    [slab[2 * y : 2 * y + 2].reshape(-1, CROP) for slab in slabs], 0
                )
                for y in (z, min(z + 1, planes - 1))
            ],
            1,
        )
        both = dot3(matrix, parts(stacked))
        out[0, z] = both[:, :CROP]
        if z + 1 < planes:
            out[0, z + 1] = both[:, CROP:]


def mark_kernel(after, out):
    del after
    out[...] = jnp.zeros(out.shape, F32)


def total_over(value, axis, size):
    if size & (size - 1):
        return lax.psum(value, axis)
    step = 1
    while step < size:
        value = value + lax.ppermute(value, axis, [(i, i ^ step) for i in range(size)])
        step *= 2
    return value


def local(frames, ref_spectrum, shifts, offsets, *, groups, devices):
    group = lax.axis_index("grp")
    device = lax.axis_index("dev")
    _, planes, ny, nx = frames.shape
    _, nz, rows, _ = ref_spectrum.shape
    total = nz * ny * nx
    factor = 1.0 / math.sqrt(total)
    half = nz // groups
    chunks = nx // LANES
    frame = frames[0]
    ints = lambda count: jnp.arange(count, dtype=jnp.int32)
    whole = lambda shape: pl.BlockSpec(shape, lambda *_: (0,) * len(shape))

    table_x = jnp.asarray(fixed_wave(nx))
    table_y = table_x if ny == nx else jnp.asarray(fixed_wave(ny))

    def send(c, *after):
        return pl.pallas_call(
            functools.partial(forward_kernel, partners=devices),
            grid_spec=pltpu.PrefetchScalarGridSpec(
                num_scalar_prefetch=1,
                grid=(planes // 2,),
                in_specs=[
                    pl.BlockSpec((2, ny, nx), lambda z, d: (z, 0, 0)),
                    pl.BlockSpec((2, 2 * nx, LANES), lambda z, d: (0, 0, c)),
                    whole((2, 2 * ny, ny)),
                ]
                + [pl.BlockSpec(memory_space=pl.ANY)] * len(after),
                out_specs=[pl.BlockSpec((2, 2, rows, LANES), lambda z, d: (0, z, 0, 0))] * devices,
                scratch_shapes=[pltpu.VMEM((2, 2, ny, LANES), F32)],
            ),
            out_shape=[jax.ShapeDtypeStruct((2, planes, rows, LANES), F32)] * devices,
        )(device_number, frame, table_x, table_y, *after)

    def exchange(pieces):
        got = list(pieces)
        for k in sorted(range(1, devices), reverse=True):
            got[k] = lax.ppermute(pieces[k], "dev", [(i, i ^ k) for i in range(devices)])
        return got

    def mark(after):
        return pl.pallas_call(
            mark_kernel,
            in_specs=[pl.BlockSpec(memory_space=pl.ANY)],
            out_shape=jax.ShapeDtypeStruct((8, LANES), F32),
        )(after)

    partner = device ^ ints(devices)
    device_number = device.astype(jnp.int32).reshape(1)
    first = send(0)
    shifts, offsets, first = lax.optimization_barrier((shifts, offsets, first))
    order = (partner[:, None] * planes + ints(planes)).reshape(-1)
    drift = lax.dynamic_index_in_dim(shifts, group, 0, keepdims=False)
    corner = lax.dynamic_index_in_dim(offsets, group, 0, keepdims=False)
    kz = (ints(nz) + group * half) % nz
    ky = device * rows + ints(rows)
    cos_z, sin_z = wave(kz, order, nz)
    split = lambda table: table.reshape(nz, devices, planes)
    table_z = halves(
        factor
        * jnp.stack(
            [
                jnp.stack([split(cos_z), split(sin_z)], 2),
                jnp.stack([-split(sin_z), split(cos_z)], 2),
            ]
        ).reshape(2 * nz, 2 * nz)
    )
    cz, sz = ramp(kz, drift[0], nz)
    turn_z = jnp.broadcast_to(jnp.stack([cz, sz])[:, :, None], (2, nz, LANES))
    cy, sy = ramp(ky, drift[1], ny)
    cx, sx = ramp(ints(nx), drift[2], nx)
    turn_yx = 0.25 * jnp.stack(
        [cy[:, None] * cx - sy[:, None] * sx, sy[:, None] * cx + cy[:, None] * sx]
    )
    ref_view = ref_spectrum.reshape(2, groups, half, rows, nx)
    group_number = group.astype(jnp.int32).reshape(1)
    steps = rows // ROWS

    def middle(gots, c, *after):
        return pl.pallas_call(
            functools.partial(middle_kernel, partners=devices, after=len(after)),
            grid_spec=pltpu.PrefetchScalarGridSpec(
                num_scalar_prefetch=1,
                grid=(steps,),
                in_specs=[
                    pl.BlockSpec((2 * planes, ROWS, LANES), lambda i, g: (0, i, 0)),
                ]
                * devices
                + [pl.BlockSpec(memory_space=pl.ANY)] * len(after)
                + [
                    whole((2, 2 * nz, 2 * nz)),
                    pl.BlockSpec((2, 1, half, ROWS, LANES), lambda i, g: (0, g[0], 0, i, c)),
                    pl.BlockSpec((2, 1, half, ROWS, LANES), lambda i, g: (0, groups - 1 - g[0], 0, i, c)),
                    whole((2, nz, LANES)),
                    pl.BlockSpec((2, ROWS, LANES), lambda i, g: (0, i, c)),
                ],
                out_specs=[
                    pl.BlockSpec((ROWS, 2, nz, LANES), lambda i, g: (i, 0, 0, 0)),
                    pl.BlockSpec((ROWS, nz, LANES), lambda i, g: (i, 0, 0)),
                    pl.BlockSpec((2, half, ROWS, LANES), lambda i, g: (0, 0, i, 0)),
                    pl.BlockSpec((2, half, ROWS, LANES), lambda i, g: (0, 0, i, 0)),
                    pl.BlockSpec((1, 8, LANES), lambda i, g: (i, 0, 0)),
                ],
            ),
            out_shape=[
                jax.ShapeDtypeStruct((rows, 2, nz, LANES), F32),
                jax.ShapeDtypeStruct((rows, nz, LANES), F32),
                jax.ShapeDtypeStruct((2, half, rows, LANES), F32),
                jax.ShapeDtypeStruct((2, half, rows, LANES), F32),
                jax.ShapeDtypeStruct((steps, 8, LANES), F32),
            ],
        )(group_number, *gots, *after, table_z, ref_view, ref_view, turn_z, turn_yx)

    crosses, sizes, owns, fars, sums = [], [], [], [], []
    swap = [(i, groups - 1 - i) for i in range(groups)]
    packed = [first]
    for c in range(chunks):
        if c + 1 < chunks:
            packed.append(send(c + 1, packed[c][0], *sums[-1:]))
        gots = [got.reshape(2 * planes, rows, LANES) for got in exchange(packed[c])]
        marks = [mark(packed[c + 1][0])] if c + 1 < chunks else []
        if 0 < c < chunks - 1:
            gots[0], fars[c - 1] = lax.optimization_barrier((gots[0], fars[c - 1]))
        cross, size, own, far, part = middle(gots, c, *marks)
        sizes.append(size)
        crosses.append(cross)
        owns.append(own)
        fars.append(lax.ppermute(far, "grp", swap))
        sums.append(part)
    mass = jnp.sum(sum(sums))
    average = total_over(mass, "dev", devices) / total

    take_x = (ints(CROP) + corner[2]) % nx
    take_y = (ints(CROP) + corner[1]) % ny
    take_z = (ints(CROP) + corner[0]) % nz
    cb, sb = wave(ints(nx), take_x, nx)
    lanes = lambda table: table.reshape(chunks, LANES, CROP)
    cb, sb = lanes(cb), lanes(sb)
    back_x = halves(
        jnp.stack(
            [jnp.concatenate([cb, sb], 2), jnp.concatenate([-sb, cb], 2)], 1
        ).reshape(2 * nx, 2 * CROP)
    )
    leaf = CROP // devices
    near = 1 << ((devices.bit_length() - 1) // 2)
    far_count = devices // near
    splits = 2 if leaf % 2 == 0 else 1
    part = leaf // splits
    turn = (ints(far_count)[None, :] * near) ^ ints(near)[:, None]
    turn = (device ^ turn).reshape(1, near, far_count, 1)
    here = ints(splits).reshape(-1, 1, 1, 1) * part + ints(part).reshape(1, 1, 1, -1)
    take_z = (turn * leaf + here + corner[0]).reshape(-1) % nz
    bz, dz = wave(take_z, kz, nz)
    back_z = halves(
        jnp.stack(
            [jnp.concatenate([bz, -dz], 1), jnp.concatenate([dz, bz], 1)], 1
        ).reshape(2 * CROP, 2 * nz)
    )
    rows_there = ((device ^ ints(near))[:, None] * rows + ints(rows)).reshape(-1)
    cos_b, sin_b = wave(take_y, rows_there, ny)
    cos_b, sin_b = cos_b.reshape(CROP, near, rows), sin_b.reshape(CROP, near, rows)
    back_y = halves(factor * jnp.stack([cos_b, -sin_b], 2)).reshape(2, CROP, -1)
    lot = 2 * far_count * part

    back = pl.pallas_call(
        functools.partial(inverse_kernel, chunks=chunks),
        grid=(steps,),
        in_specs=[pl.BlockSpec(memory_space=pltpu.SMEM)]
        + [pl.BlockSpec((ROWS, 2, nz, LANES), lambda i: (i, 0, 0, 0))] * chunks
        + [pl.BlockSpec((ROWS, nz, LANES), lambda i: (i, 0, 0))] * chunks
        + [whole((2, 2 * nx, 2 * CROP)), whole((2, 2 * CROP, 2 * nz))],
        out_specs=[pl.BlockSpec((lot, ROWS, LANES), lambda i: (0, i, 0))] * (splits * near),
        out_shape=[jax.ShapeDtypeStruct((lot, rows, LANES), F32)] * (splits * near),
    )(average.reshape(1), *crosses, *sizes, back_x, back_z)

    def partial(slabs, *after):
        return pl.pallas_call(
            functools.partial(partial_kernel, near=near),
            grid=(far_count,),
            in_specs=[whole(back_y.shape)]
            + [pl.BlockSpec((2 * part, rows, CROP), lambda f: (f, 0, 0))] * near
            + [pl.BlockSpec(memory_space=pl.ANY)] * len(after),
            out_specs=pl.BlockSpec((1, part, CROP, CROP), lambda f: (f, 0, 0, 0)),
            out_shape=jax.ShapeDtypeStruct((far_count, part, CROP, CROP), F32),
        )(back_y, *slabs, *after)

    new_reference = jnp.concatenate([own + far for own, far in zip(owns, fars)], 3)
    gathered = []
    for h in range(splits):
        slabs = list(back[h * near : (h + 1) * near])
        for k in range(1, near):
            slabs[k] = lax.ppermute(slabs[k], "dev", [(i, i ^ k) for i in range(devices)])
        gathered.append(slabs)
    fields = []
    for h in range(splits):
        sums_y = partial(gathered[h], *([new_reference] if h else []))
        field = sums_y[0]
        moved = [
            lax.ppermute(sums_y[k], "dev", [(i, i ^ (k * near)) for i in range(devices)])
            for k in range(1, far_count)
        ]
        fields.append(field + sum(moved))
    field = jnp.concatenate(fields, 0)
    return (field[None], new_reference)


def solution(mesh):
    body = functools.partial(local, groups=mesh.shape["grp"], devices=mesh.shape["dev"])
    return jax.shard_map(
        body,
        mesh=mesh,
        in_specs=(P("grp", "dev", None, None), P(None, None, "dev", None), P(), P()),
        out_specs=(P("grp", "dev", None, None), P(None, "grp", "dev", None)),
        check_vma=False,
    )
```

```python
import functools
import math

import jax
import jax.numpy as jnp
import ml_dtypes
import numpy as np
from jax import lax
from jax.experimental import pallas as pl
from jax.experimental.pallas import tpu as pltpu
from jax.sharding import PartitionSpec as P


CROP = 128
LANES = 128
ROWS = 8
F32 = jnp.float32
BF16 = jnp.bfloat16


def fixed_table(phases, length):
    angles = 2.0 * np.pi / length * (phases % length)
    table = np.concatenate([np.cos(angles), np.sin(angles)], 0).astype(np.float32)
    high = table.astype(ml_dtypes.bfloat16)
    low = (table - high.astype(np.float32)).astype(ml_dtypes.bfloat16)
    return np.stack([high, low])


def fixed_wave(length):
    return fixed_table(np.outer(np.arange(length), np.arange(length)), length)


def fixed_folds(length):
    samples = np.arange(length // 2)
    pick = [np.outer(np.arange(odd, length, 2), samples) for odd in (0, 1)]
    return np.stack([fixed_table(phases, length) for phases in pick])


def wave(rows, columns, length):
    phases = rows[:, None] * columns[None, :] % length
    angles = 2.0 * math.pi / length * phases.astype(F32)
    return (jnp.cos(angles), jnp.sin(angles))


def ramp(index, drift, length):
    angles = 2.0 * math.pi / length * (index * drift % length).astype(F32)
    return (jnp.cos(angles), jnp.sin(angles))


def halves(table):
    high = lax.reduce_precision(table, 8, 7)
    return jnp.stack([high.astype(BF16), (table - high).astype(BF16)])


def parts(value):
    high = value.astype(BF16)
    return high, (value - high.astype(F32)).astype(BF16)


def dot3(left, right):
    return jnp.dot(
        jnp.concatenate([left[0], left[0], left[1]], 1),
        jnp.concatenate([right[0], right[1], right[0]], 0),
        preferred_element_type=F32,
    )


def forward_kernel(device, frame, table_x, table_y, *refs, partners):
    outs, scratch = refs[-1 - partners : -1], refs[-1]
    count, ny, nx = frame.shape
    rows = outs[0].shape[2]
    column = [jnp.concatenate([table_x[i, :nx, :], table_x[i, nx:, :]], 1) for i in range(2)]
    fold = ny // 2
    lines = [[scratch.at[z, p] for p in range(2)] for z in range(count)]
    for z in range(count):
        plane = dot3(parts(frame[z]), column)
        top, bottom = plane[:fold], plane[fold:]
        for odd, side in enumerate((top + bottom, top - bottom)):
            both = dot3((table_y[odd, 0], table_y[odd, 1]), parts(side))
            where = pl.ds(odd, fold, stride=2)
            lines[z][0][where, :] = both[:fold, :LANES] - both[fold:, LANES:]
            lines[z][1][where, :] = -both[:fold, LANES:] - both[fold:, :LANES]
    for k, out in enumerate(outs):
        at = pl.ds(pl.multiple_of((device[0] ^ k) * rows, rows), rows)
        for z in range(count):
            out[0, z] = scratch[z, 0, at, :]
            out[1, z] = scratch[z, 1, at, :]


def middle_kernel(group, *refs, partners, after):
    del group
    refs = refs[:partners] + refs[partners + after :]
    gots, (table, ref_own, ref_far, turn_z, turn_yx, cross, size, own, far, sums) = refs[:-10], refs[-10:]
    each = gots[0].shape[0]
    nz = cross.shape[2]
    half = own.shape[1]
    flats = [got.reshape(each * ROWS, LANES) for got in gots]
    near = ref_own.reshape(2 * half * ROWS, LANES)
    away = ref_far.reshape(2 * half * ROWS, LANES)
    own_flat = own.reshape(2 * half * ROWS, LANES)
    far_flat = far.reshape(2 * half * ROWS, LANES)
    matrix = (table[0], table[1])
    zc, zs = turn_z[0], turn_z[1]
    total = jnp.zeros((8, LANES), F32)
    for pair in range(0, ROWS, 2):
        taken = [
            jnp.concatenate([flat[pl.ds(r, each, stride=ROWS), :] for flat in flats], 0)
            for r in (pair, pair + 1)
        ]
        freq = dot3(matrix, parts(jnp.concatenate(taken, 1)))
        for r in (pair, pair + 1):
            at = slice((r - pair) * LANES, (r - pair + 1) * LANES)
            fr, fi = freq[:nz, at], freq[nz:, at]
            yc, ys = turn_yx[0, r : r + 1, :], turn_yx[1, r : r + 1, :]
            ar, ai = fr * zc + fi * zs, fi * zc - fr * zs
            wr, wi = ar * yc + ai * ys, ai * yc - ar * ys
            own_part = [near[pl.ds(p * half * ROWS + r, half, stride=ROWS), :] for p in range(2)]
            far_part = [away[pl.ds(p * half * ROWS + r, half, stride=ROWS), :] for p in range(2)]
            for p, w in enumerate((wr, wi)):
                where = pl.ds(p * half * ROWS + r, half, stride=ROWS)
                own_flat[where, :] = w[:half] + 0.5 * own_part[p]
                far_flat[where, :] = w[half:]
            rr = jnp.concatenate([own_part[0], far_part[0]], 0)
            ri = jnp.concatenate([own_part[1], far_part[1]], 0)
            cr = fr * rr + fi * ri
            ci = fi * rr - fr * ri
            cross[r, 0] = cr
            cross[r, 1] = ci
            magnitude = jnp.sqrt(cr * cr + ci * ci)
            size[r] = magnitude
            total = total + jnp.sum(magnitude.reshape(nz // 8, 8, LANES), 0)
    sums[0] = total


def inverse_kernel(average, *refs, chunks):
    crosses, sizes = refs[:chunks], refs[chunks : 2 * chunks]
    table_x, table_z = refs[2 * chunks : 2 * chunks + 2]
    outs = refs[2 * chunks + 2 :]
    each = outs[0].shape[0]
    nz = crosses[0].shape[2]
    mean = average[0]
    flats = [out.reshape(each * ROWS, LANES) for out in outs]
    matrix = (table_z[0], table_z[1])
    width = None
    for c, (cross, size) in enumerate(zip(crosses, sizes)):
        scale = 1.0 / (size[...] + mean)
        white = jnp.concatenate(
            [(cross[:, p] * scale).reshape(ROWS * nz, LANES) for p in range(2)], 1
        )
        at = slice(c * 2 * LANES, (c + 1) * 2 * LANES)
        piece = dot3(parts(white), (table_x[0, at, :], table_x[1, at, :]))
        width = piece if width is None else width + piece
    for pair in range(0, ROWS, 2):
        stacked = jnp.concatenate(
            [
                jnp.concatenate([width[r * nz : (r + 1) * nz, :CROP], width[r * nz : (r + 1) * nz, CROP:]], 0)
                for r in (pair, pair + 1)
            ],
            1,
        )
        depth = dot3(matrix, parts(stacked))
        for k, flat in enumerate(flats):
            at = slice(k * each, (k + 1) * each)
            flat[pl.ds(pair, each, stride=ROWS), :] = depth[at, :CROP]
            flat[pl.ds(pair + 1, each, stride=ROWS), :] = depth[at, CROP:]


def partial_kernel(table, *refs, near, far):
    slabs, outs = refs[:near], refs[-far:]
    planes = outs[0].shape[0]
    matrix = (table[0], table[1])
    for f, out in enumerate(outs):
        for z in range(0, planes, 2):
            stacked = jnp.concatenate(
                [
                    jnp.concatenate(
                        [slab[f, 2 * y : 2 * y + 2].reshape(-1, CROP) for slab in slabs], 0
                    )
                    for y in (z, min(z + 1, planes - 1))
                ],
                1,
            )
            both = dot3(matrix, parts(stacked))
            out[z] = both[:, :CROP]
            if z + 1 < planes:
                out[z + 1] = both[:, CROP:]


def merge_kernel(*refs):
    owns, fars, out = refs[:2], refs[2:4], refs[-1]
    for i, (own, far) in enumerate(zip(owns, fars)):
        out[..., i * LANES : (i + 1) * LANES] = own[...] + far[...]


def mark_kernel(after, out):
    del after
    out[...] = jnp.zeros(out.shape, F32)


def total_over(value, axis, size):
    if size & (size - 1):
        return lax.psum(value, axis)
    step = 1
    while step < size:
        value = value + lax.ppermute(value, axis, [(i, i ^ step) for i in range(size)])
        step *= 2
    return value


def local(frames, ref_spectrum, shifts, offsets, *, groups, devices):
    group = lax.axis_index("grp")
    device = lax.axis_index("dev")
    _, planes, ny, nx = frames.shape
    _, nz, rows, _ = ref_spectrum.shape
    total = nz * ny * nx
    factor = 1.0 / math.sqrt(total)
    half = nz // groups
    chunks = nx // LANES
    frame = frames[0]
    ints = lambda count: jnp.arange(count, dtype=jnp.int32)
    whole = lambda shape: pl.BlockSpec(shape, lambda *_: (0,) * len(shape))

    table_x = jnp.asarray(fixed_wave(nx))
    table_y = jnp.asarray(fixed_folds(ny))

    def send(c, *after):
        return pl.pallas_call(
            functools.partial(forward_kernel, partners=devices),
            grid_spec=pltpu.PrefetchScalarGridSpec(
                num_scalar_prefetch=1,
                grid=(planes // 2,),
                in_specs=[
                    pl.BlockSpec((2, ny, nx), lambda z, d: (z, 0, 0)),
                    pl.BlockSpec((2, 2 * nx, LANES), lambda z, d: (0, 0, c)),
                    whole((2, 2, ny, ny // 2)),
                ]
                + [pl.BlockSpec(memory_space=pl.ANY)] * len(after),
                out_specs=[pl.BlockSpec((2, 2, rows, LANES), lambda z, d: (0, z, 0, 0))] * devices,
                scratch_shapes=[pltpu.VMEM((2, 2, ny, LANES), F32)],
            ),
            out_shape=[jax.ShapeDtypeStruct((2, planes, rows, LANES), F32)] * devices,
        )(device_number, frame, table_x, table_y, *after)

    def exchange(pieces):
        got = list(pieces)
        for k in sorted(range(1, devices), reverse=True):
            got[k] = lax.ppermute(pieces[k], "dev", [(i, i ^ k) for i in range(devices)])
        return got

    def mark(after):
        return pl.pallas_call(
            mark_kernel,
            in_specs=[pl.BlockSpec(memory_space=pl.ANY)],
            out_shape=jax.ShapeDtypeStruct((8, LANES), F32),
        )(after)

    partner = device ^ ints(devices)
    device_number = device.astype(jnp.int32).reshape(1)
    first = send(0)
    shifts, offsets, first = lax.optimization_barrier((shifts, offsets, first))
    order = (partner[:, None] * planes + ints(planes)).reshape(-1)
    drift = lax.dynamic_index_in_dim(shifts, group, 0, keepdims=False)
    corner = lax.dynamic_index_in_dim(offsets, group, 0, keepdims=False)
    kz = (ints(nz) + group * half) % nz
    ky = device * rows + ints(rows)
    cos_z, sin_z = wave(kz, order, nz)
    split = lambda table: table.reshape(nz, devices, planes)
    table_z = halves(
        factor
        * jnp.stack(
            [
                jnp.stack([split(cos_z), split(sin_z)], 2),
                jnp.stack([-split(sin_z), split(cos_z)], 2),
            ]
        ).reshape(2 * nz, 2 * nz)
    )
    cz, sz = ramp(kz, drift[0], nz)
    turn_z = jnp.broadcast_to(jnp.stack([cz, sz])[:, :, None], (2, nz, LANES))
    cy, sy = ramp(ky, drift[1], ny)
    cx, sx = ramp(ints(nx), drift[2], nx)
    turn_yx = 0.25 * jnp.stack(
        [cy[:, None] * cx - sy[:, None] * sx, sy[:, None] * cx + cy[:, None] * sx]
    )
    ref_view = ref_spectrum.reshape(2, groups, half, rows, nx)
    group_number = group.astype(jnp.int32).reshape(1)
    steps = rows // ROWS

    def merge(pair, *into):
        piece = pl.BlockSpec((2, half, ROWS, LANES), lambda i: (0, 0, i, 0))
        at = slice(2 * pair, 2 * pair + 2)
        return pl.pallas_call(
            merge_kernel,
            grid=(steps,),
            in_specs=[piece] * 4 + [pl.BlockSpec(memory_space=pl.ANY)] * len(into),
            out_specs=pl.BlockSpec((2, half, ROWS, 2 * LANES), lambda i: (0, 0, i, pair)),
            out_shape=jax.ShapeDtypeStruct((2, half, rows, nx), F32),
            input_output_aliases={4: 0} if into else {},
        )(*owns[at], *fars[at], *into)

    def middle(gots, c, *after):
        return pl.pallas_call(
            functools.partial(middle_kernel, partners=devices, after=len(after)),
            grid_spec=pltpu.PrefetchScalarGridSpec(
                num_scalar_prefetch=1,
                grid=(steps,),
                in_specs=[
                    pl.BlockSpec((2 * planes, ROWS, LANES), lambda i, g: (0, i, 0)),
                ]
                * devices
                + [pl.BlockSpec(memory_space=pl.ANY)] * len(after)
                + [
                    whole((2, 2 * nz, 2 * nz)),
                    pl.BlockSpec((2, 1, half, ROWS, LANES), lambda i, g: (0, g[0], 0, i, c)),
                    pl.BlockSpec((2, 1, half, ROWS, LANES), lambda i, g: (0, groups - 1 - g[0], 0, i, c)),
                    whole((2, nz, LANES)),
                    pl.BlockSpec((2, ROWS, LANES), lambda i, g: (0, i, c)),
                ],
                out_specs=[
                    pl.BlockSpec((ROWS, 2, nz, LANES), lambda i, g: (i, 0, 0, 0)),
                    pl.BlockSpec((ROWS, nz, LANES), lambda i, g: (i, 0, 0)),
                    pl.BlockSpec((2, half, ROWS, LANES), lambda i, g: (0, 0, i, 0)),
                    pl.BlockSpec((2, half, ROWS, LANES), lambda i, g: (0, 0, i, 0)),
                    pl.BlockSpec((1, 8, LANES), lambda i, g: (i, 0, 0)),
                ],
            ),
            out_shape=[
                jax.ShapeDtypeStruct((rows, 2, nz, LANES), F32),
                jax.ShapeDtypeStruct((rows, nz, LANES), F32),
                jax.ShapeDtypeStruct((2, half, rows, LANES), F32),
                jax.ShapeDtypeStruct((2, half, rows, LANES), F32),
                jax.ShapeDtypeStruct((steps, 8, LANES), F32),
            ],
        )(group_number, *gots, *after, table_z, ref_view, ref_view, turn_z, turn_yx)

    crosses, sizes, owns, fars, sums = [], [], [], [], []
    swap = [(i, groups - 1 - i) for i in range(groups)]
    packed = [first]
    for c in range(chunks):
        if c + 1 < chunks:
            packed.append(send(c + 1, packed[c][0], *sums[-1:]))
        gots = [got.reshape(2 * planes, rows, LANES) for got in exchange(packed[c])]
        marks = [mark(packed[c + 1][0])] if c + 1 < chunks else []
        if 0 < c < chunks - 1:
            gots[0], fars[c - 1] = lax.optimization_barrier((gots[0], fars[c - 1]))
        if c == chunks - 1:
            new_reference = []
            for pair in range(chunks // 2 - 1):
                new_reference = [merge(pair, *new_reference)]
            marks = marks + new_reference
        cross, size, own, far, part = middle(gots, c, *marks)
        sizes.append(size)
        crosses.append(cross)
        owns.append(own)
        fars.append(lax.ppermute(far, "grp", swap))
        sums.append(part)
    mass = jnp.sum(sum(sums))
    average = total_over(mass, "dev", devices) / total

    take_x = (ints(CROP) + corner[2]) % nx
    take_y = (ints(CROP) + corner[1]) % ny
    take_z = (ints(CROP) + corner[0]) % nz
    cb, sb = wave(ints(nx), take_x, nx)
    lanes = lambda table: table.reshape(chunks, LANES, CROP)
    cb, sb = lanes(cb), lanes(sb)
    back_x = halves(
        jnp.stack(
            [jnp.concatenate([cb, sb], 2), jnp.concatenate([-sb, cb], 2)], 1
        ).reshape(2 * nx, 2 * CROP)
    )
    leaf = CROP // devices
    near = 1 << ((devices.bit_length() - 1) // 2)
    far_count = devices // near
    splits = math.gcd(leaf, 2)
    part = leaf // splits
    turn = (ints(far_count)[None, :] * near) ^ ints(near)[:, None]
    turn = (device ^ turn).reshape(1, near, far_count, 1)
    here = ints(splits).reshape(-1, 1, 1, 1) * part + ints(part).reshape(1, 1, 1, -1)
    take_z = (turn * leaf + here + corner[0]).reshape(-1) % nz
    bz, dz = wave(take_z, kz, nz)
    back_z = halves(
        jnp.stack(
            [jnp.concatenate([bz, -dz], 1), jnp.concatenate([dz, bz], 1)], 1
        ).reshape(2 * CROP, 2 * nz)
    )
    rows_there = ((device ^ ints(near))[:, None] * rows + ints(rows)).reshape(-1)
    cos_b, sin_b = wave(take_y, rows_there, ny)
    cos_b, sin_b = cos_b.reshape(CROP, near, rows), sin_b.reshape(CROP, near, rows)
    back_y = halves(factor * jnp.stack([cos_b, -sin_b], 2)).reshape(2, CROP, -1)
    lot = 2 * far_count * part

    back = pl.pallas_call(
        functools.partial(inverse_kernel, chunks=chunks),
        grid=(steps,),
        in_specs=[pl.BlockSpec(memory_space=pltpu.SMEM)]
        + [pl.BlockSpec((ROWS, 2, nz, LANES), lambda i: (i, 0, 0, 0))] * chunks
        + [pl.BlockSpec((ROWS, nz, LANES), lambda i: (i, 0, 0))] * chunks
        + [whole((2, 2 * nx, 2 * CROP)), whole((2, 2 * CROP, 2 * nz))],
        out_specs=[pl.BlockSpec((lot, ROWS, LANES), lambda i: (0, i, 0))] * (splits * near),
        out_shape=[jax.ShapeDtypeStruct((lot, rows, LANES), F32)] * (splits * near),
    )(average.reshape(1), *crosses, *sizes, back_x, back_z)

    def partial(slabs, *after):
        step = 2 if part % 2 == 0 else 1
        views = [slab.reshape(far_count, 2 * part, rows, CROP) for slab in slabs]
        return pl.pallas_call(
            functools.partial(partial_kernel, near=near, far=far_count),
            grid=(part // step,),
            in_specs=[whole(back_y.shape)]
            + [pl.BlockSpec((far_count, 2 * step, rows, CROP), lambda z: (0, z, 0, 0))] * near
            + [pl.BlockSpec(memory_space=pl.ANY)] * len(after),
            out_specs=[pl.BlockSpec((step, CROP, CROP), lambda z: (z, 0, 0))] * far_count,
            out_shape=[jax.ShapeDtypeStruct((part, CROP, CROP), F32)] * far_count,
        )(back_y, *views, *after)

    gathered = []
    for h in range(splits):
        slabs = list(back[h * near : (h + 1) * near])
        for k in range(1, near):
            slabs[k] = lax.ppermute(slabs[k], "dev", [(i, i ^ k) for i in range(devices)])
        gathered.append(slabs)
    fields, order_y = [], []
    for h in range(splits):
        sums_y = partial(gathered[h], *order_y)
        order_y = [sums_y[0]]
        field = sums_y[0]
        moved = [
            lax.ppermute(sums_y[k], "dev", [(i, i ^ (k * near)) for i in range(devices)])
            for k in range(1, far_count)
        ]
        fields.append(field + sum(moved))
    field = jnp.concatenate(fields, 0)
    new_reference = merge(chunks // 2 - 1, *new_reference)
    return (field[None], new_reference)


def solution(mesh):
    body = functools.partial(local, groups=mesh.shape["grp"], devices=mesh.shape["dev"])
    return jax.shard_map(
        body,
        mesh=mesh,
        in_specs=(P("grp", "dev", None, None), P(None, None, "dev", None), P(), P()),
        out_specs=(P("grp", "dev", None, None), P(None, "grp", "dev", None)),
        check_vma=False,
    )
```
